32 devices in a mesh: rep: 2 (over x), exp: 16 (over z, y, core).
Axes of the slice: x: 2, y: 2, z: 4, core: 2. Of those that a mesh axis runs over, the one named last changes fastest.
Arguments:
- a_tokens: bfloat16 [64, 7168], P(('rep', 'exp')), parts along dimension 0, may hold values from -6 to 6
- a_gain: float32 [7168], replicated, may hold values from 0.25 to 1.75
- dense_gate: bfloat16 [7168, 18432], P(None, 'exp'), may hold values from -0.0625 to 0.0625
- dense_up: bfloat16 [7168, 18432], P(None, 'exp'), may hold values from -0.0625 to 0.0625
- dense_down: bfloat16 [18432, 7168], P('exp'), may hold values from -0.046875 to 0.046875
- b_tokens: bfloat16 [128, 7168], P(('rep', 'exp')), parts along dimension 0, may hold values from -6 to 6
- b_gain: float32 [7168], replicated, may hold values from 0.25 to 1.75
- expert_ids: int32 [128, 8], P(('rep', 'exp')), parts along dimension 0, may hold values from 0 to 15, all different within a row; in each aligned block of 4 rows (0 to 3, 4 to 7, ...) at most 3 rows name the same one
- route_weights: float32 [128, 8], P(('rep', 'exp')), parts along dimension 0, may hold values from 0.05 to 0.5
- expert_gate: bfloat16 [16, 7168, 1024], P('exp'), may hold values from -0.0625 to 0.0625
- expert_up: bfloat16 [16, 7168, 1024], P('exp'), may hold values from -0.0625 to 0.0625
- expert_down: bfloat16 [16, 1024, 7168], P('exp'), may hold values from -0.1875 to 0.1875
Outputs:
- a_out: bfloat16 [64, 7168], P(('rep', 'exp')), parts along dimension 0
- b_out: bfloat16 [128, 7168], P(('rep', 'exp')), parts along dimension 0
The draws below stay inside these ranges and needn't reach their ends.
There are 2 independent parts, one for each index of `rep`. The reference program is written for one: setup_inputs(seed, part) draws one part's arguments, and reference() takes and returns one part's arrays. A program takes and returns all parts, laid end to end along the dimension named above; an argument that names none is the same for every part. Nothing has to cross between parts.
Inputs may be any that keep to these rules, and one draw needn't show every extreme that they name: `expert_ids`: each row names 8 different experts. Among the rows of one device no expert is named more than 3 times, and in some devices one expert is named exactly 3 times.
All inputs are finite; a program needn't handle non-finite values.
Results may differ from the reference program's by a relative error of at most 0.008.
Values may be sent and summed in bfloat16 or wider, within the bound.
A program may use at most 192 MiB of HBM per device.

```python
import math
import jax
import jax.numpy as jnp
import numpy as np
from jax import lax

D = 7168
FF = 18432
EH = 1024
EXPERTS = 16
TOPK = 8
TB_DEV = 4
TA = 32
TB = 64
GROUP = 1
ES = 1024
CAP = 3


def levels(stream_key, extent, pieces, low, high):
    def one(position, parts):
        draws = jax.random.uniform(jax.random.fold_in(jax.random.fold_in(stream_key, 6), position), (parts,), jnp.float32, low / len(pieces), high / len(pieces))
        return jnp.repeat(jnp.exp(draws), extent[position] // parts).reshape((-1,) + (1,) * (len(extent) - position - 1))

    level = one(*pieces[0])
    for cut in pieces[1:]:
        level = level * one(*cut)
    return level


def shared_out(stream_key, own, number, rows, amount, top, bound, slope):
    order = jax.random.permutation(stream_key, amount)
    packed, ordinary = load_shares(amount, rows * top, bound, slope, True), load_shares(amount, rows * top, bound, slope, False)
    places = jnp.arange(amount)

    def named(sizes, offset_by):
        used = int((sizes > 0).sum())
        fixed = max(1, used // 4)
        shifted = fixed + (places - fixed + offset_by * (used - fixed)) % max(1, amount - fixed)
        return jnp.zeros((amount,), jnp.int32).at[order[jnp.where(places < fixed, places, shifted)]].set(jnp.asarray(sizes, jnp.int32))

    sizes = jnp.where(number % 4 == 0, named(packed, number // 4), named(ordinary, number - number // 4 - 1))
    mixed = jax.random.permutation(jax.random.fold_in(own, 3), amount)
    donor, receiver = mixed[0:amount // 2 * 2:2], mixed[1:amount // 2 * 2:2]
    slack = jnp.minimum(sizes[donor] - 1, bound - sizes[receiver]) // 2
    slack = jnp.where((donor == order[0]) | (receiver == order[0]) | (sizes[receiver] == 0), 0, jnp.maximum(slack, 0))
    shifted = jax.random.randint(jax.random.fold_in(own, 4), (amount // 2,), 0, 1 << 20) % (slack + 1)
    sizes = sizes.at[donor].add(-shifted).at[receiver].add(shifted)
    labels = jnp.searchsorted(jnp.cumsum(sizes), jnp.arange(rows * top), side="right").astype(jnp.int32)
    table = labels.reshape(top, rows).T
    table = table[jax.random.permutation(jax.random.fold_in(own, 1), rows)]
    offset_by = jax.random.randint(jax.random.fold_in(own, 2), (rows, 1), 0, top)
    return jnp.take_along_axis(table, (jnp.arange(top)[None, :] + offset_by) % top, axis=1)


def load_shares(amount, total, reach, skew, full):
    portions = [(1 << 20) // math.isqrt(grade ** skew) + 1 for grade in range(1, amount + 1)]
    largest = reach if full else min(reach, max(-(-total // amount), total * portions[0] // sum(portions)))
    least = 1 if total - largest >= amount - 1 else 0
    counts, spare = [largest] + [least] * (amount - 1), total - largest - least * (amount - 1)
    while spare > 0:
        candidates = [i for i in range(1, amount) if counts[i] < largest] or [i for i in range(1, amount) if counts[i] < reach]
        whole, left = sum([portions[i] for i in candidates]), spare
        for i in candidates:
            more = min(reach - counts[i], max(1, left * portions[i] // whole), spare)
            counts[i] = counts[i] + more
            spare = spare - more
    return np.array(counts)


def noise(stream_key, shape, scale, most, cuts=(), kind=jnp.bfloat16):
    values = jax.random.normal(stream_key, shape, jnp.float32) * scale
    if len(cuts) > 0:
        values = levels(stream_key, shape, cuts, -0.22, 0.18) * values
    return jnp.clip(values, min=-most, max=most).astype(kind)


def setup_inputs(seed: int = 0, part: int = 0) -> dict:
    splits = jax.random.split(jax.random.key(seed), 13)
    own_keys = jax.random.split(jax.random.fold_in(splits[12], part), 13)
    a_tokens = noise(own_keys[0], (TA, D), 1.0, 6.0, ((0, 16),))
    a_gain = jnp.clip(1.0 + 0.15 * jax.random.normal(splits[1], (D,), jnp.float32), 0.25, 1.75)
    dense_gate = noise(splits[2], (D, FF), D ** -0.5, 0.0625, ((1, 16),))
    dense_up = noise(splits[3], (D, FF), D ** -0.5, 0.0625, ((1, 16),))
    dense_down = noise(splits[4], (FF, D), FF ** -0.5, 0.046875, ((0, 16),))
    b_tokens = noise(own_keys[5], (TB, D), 1.0, 6.0, ((0, 16),))
    b_gain = jnp.clip(1.0 + 0.15 * jax.random.normal(splits[6], (D,), jnp.float32), 0.25, 1.75)
    expert_ids_keys = jax.random.split(jax.random.fold_in(own_keys[7], 1), TB // TB_DEV)
    expert_ids_turns = jax.random.permutation(jax.random.fold_in(own_keys[7], 3), TB // TB_DEV)
    expert_ids = jax.vmap(lambda own, number: shared_out(jax.random.fold_in(own_keys[7], 2), own, number, TB_DEV, EXPERTS, TOPK, CAP, 2))(expert_ids_keys, expert_ids_turns).reshape((TB, TOPK))
    route_weights = jnp.clip(jnp.exp(math.log(0.5) - 2.3025851 * jax.random.uniform(own_keys[8], (TB, TOPK), jnp.float32) ** levels(own_keys[8], (TB, TOPK), ((0, 16),), -0.2, 0.2)), 0.05, 0.5)
    expert_gate = noise(splits[9], (EXPERTS * GROUP, D, ES), D ** -0.5, 0.0625, ((0, 16),))
    expert_up = noise(splits[10], (EXPERTS * GROUP, D, ES), D ** -0.5, 0.0625, ((0, 16),))
    expert_down = noise(splits[11], (EXPERTS * GROUP, ES, D), EH ** -0.5, 0.1875, ((0, 16),))
    return dict(a_tokens=a_tokens, a_gain=a_gain, dense_gate=dense_gate, dense_up=dense_up, dense_down=dense_down, b_tokens=b_tokens, b_gain=b_gain, expert_ids=expert_ids, route_weights=route_weights, expert_gate=expert_gate, expert_up=expert_up, expert_down=expert_down)


def normed(values, gain_vec):
    return values * lax.rsqrt(lax.optimization_barrier(jnp.mean(values * values, axis=-1, keepdims=True)) + 1e-06) * gain_vec

def reference(a_tokens, a_gain, dense_gate, dense_up, dense_down, b_tokens, b_gain, expert_ids, route_weights, expert_gate, expert_up, expert_down):
    a_float = a_tokens.astype(jnp.float32)
    a_normed = normed(a_float, a_gain).astype(jnp.bfloat16)
    gate_proj = jnp.dot(a_normed, dense_gate, preferred_element_type=jnp.float32)
    up_proj = jnp.dot(a_normed, dense_up, preferred_element_type=jnp.float32)
    hidden = (jax.nn.silu(gate_proj) * up_proj).astype(jnp.bfloat16)
    a_out = (a_float + jnp.dot(hidden, dense_down, preferred_element_type=jnp.float32)).astype(jnp.bfloat16)
    b_float = b_tokens.astype(jnp.float32)
    b_normed = normed(b_float, b_gain).astype(jnp.bfloat16)
    b_wide = b_normed.astype(jnp.float32)
    onehot = (expert_ids[:, :, None] == jnp.arange(EXPERTS, dtype=jnp.int32)[None, None, :]).astype(jnp.float32)
    mix_table = jnp.einsum('tk,tke->et', route_weights.astype(jnp.float32), onehot)
    gate_blocks = expert_gate.reshape(EXPERTS, GROUP, D, ES)
    up_blocks = expert_up.reshape(EXPERTS, GROUP, D, ES)
    down_blocks = expert_down.reshape(EXPERTS, GROUP, ES, D)

    def one_expert(running, inputs):
        w_gate, w_up, w_down, weight = inputs
        gate_e = jnp.einsum('td,gds->tgs', b_wide, w_gate.astype(jnp.float32))
        up_e = jnp.einsum('td,gds->tgs', b_wide, w_up.astype(jnp.float32))
        hid_e = (jax.nn.silu(gate_e) * up_e).astype(jnp.bfloat16)
        partial_value = jnp.einsum('tgs,gsd->tgd', hid_e.astype(jnp.float32), w_down.astype(jnp.float32)).astype(jnp.bfloat16)
        expert_out = lax.optimization_barrier(jnp.sum(partial_value.astype(jnp.float32), axis=1)).astype(jnp.bfloat16)
        return (running + weight[:, None] * expert_out.astype(jnp.float32), None)
    totals, _ = lax.scan(one_expert, jnp.zeros((TB, D), jnp.float32), (gate_blocks, up_blocks, down_blocks, mix_table))
    b_out = (b_float + totals).astype(jnp.bfloat16)
    return (a_out, b_out)
```

```python
import functools

import jax
import jax.numpy as jnp
from jax import lax
from jax.experimental import pallas as pl
from jax.experimental.pallas import tpu as pltpu
from jax.sharding import PartitionSpec as P

EXPERTS = 16
LANES = 128
F32 = jnp.float32
BF16 = jnp.bfloat16
MESH = pl.DeviceIdType.MESH


def pick(total, sizes):
    for size in sizes:
        if total % size == 0:
            return size
    return total


def factor(chips):
    inner = 1
    while inner * inner * 4 <= chips and chips % (inner * 2) == 0:
        inner *= 2
    return chips // inner, inner


def normed(values, gain_row):
    mean = jnp.mean(values * values, axis=-1, keepdims=True)
    return values * lax.rsqrt(mean + 1e-06) * gain_row


def drain(ref, sem):
    pltpu.make_async_copy(ref, ref, sem).wait()


def kernel(
    n, kq, kc, cb, cw,
    a_hbm, ag_hbm, b_hbm, bg_hbm, ids_hbm, rw_hbm,
    dg_hbm, du_hbm, dd_hbm, eg_hbm, eu_hbm, ed_hbm,
    a_out, b_out,
    a_in, ag_in, b_in, bg_in, ids_in, rw_in,
    gu, dn, gat_b, gat_a, g_acc, u_acc, hid_b, hid_a,
    back_b, back_a,
    in_sem, gu_sem, dn_sem,
    gz_send, gz_recv, gy_send, gy_recv, gc_send, gc_recv,
    s1_send, s1_recv, s2_send, s2_recv, s3_send, s3_recv,
):
    me = lax.axis_index("exp")
    core = lax.rem(me, 2)
    chip = me // 2
    chips = n // 2
    outer, inner = factor(chips)
    p = chip // inner
    q = lax.rem(chip, inner)
    expert = me // (n // EXPERTS)
    rows_a, width = a_in.shape
    rows_b = b_in.shape[0]
    steps = width // kq
    slots = width // cb
    chunks = width // cw
    es = eg_hbm.shape[2]
    fd = dg_hbm.shape[1]
    front = width // 2
    wide = gat_b.shape[3]
    sibling = {"exp": chip * 2 + (1 - core)}

    def line(d):
        return {"exp": (lax.rem(p + d + outer, outer) * inner + q) * 2 + core}

    def cross(e):
        return {"exp": (p * inner + lax.rem(q + e + inner, inner)) * 2 + core}

    def cols(j, size):
        return pl.ds(pl.multiple_of(j * size, size), size)

    def loop(low, high, body):
        def go(i, carry):
            body(i)
            return carry

        lax.fori_loop(low, high, go, 0)

    def signal(target):
        pl.semaphore_signal(barrier, inc=1, device_id=target, device_id_type=MESH)

    barrier = pltpu.get_barrier_semaphore()
    loop(1, outer, lambda d: signal(line(d)))
    loop(1, inner, lambda e: signal(cross(e)))
    signal(sibling)

    inputs = [
        pltpu.make_async_copy(src, dst, in_sem.at[i])
        for i, (src, dst) in enumerate((
            (b_hbm, b_in), (bg_hbm, bg_in), (ids_hbm, ids_in),
            (rw_hbm, rw_in), (a_hbm, a_in), (ag_hbm, ag_in),
        ))
    ]
    for copy in inputs:
        copy.start()

    def gu_slot(ph, w, i):
        return gu.at[w, i, :, pl.ds(0, (es, fd)[ph])]

    def gu_copy(ph, w, i):
        if ph == 0:
            src = (eg_hbm, eu_hbm)[w].at[0, cols(i, kq), :]
        else:
            src = (dg_hbm, du_hbm)[w].at[cols(i, kq), :]
        return pltpu.make_async_copy(src, gu_slot(ph, w, i), gu_sem.at[w, i])

    def dn_place(ph, j):
        return j if ph == 0 else (j + slots) % (slots + slots // 2)

    def dn_slot(ph, j):
        return dn.at[dn_place(ph, j), pl.ds(0, (es, fd)[ph])]

    def dn_copy(ph, j):
        src = ed_hbm.at[0, :, cols(j, cb)] if ph == 0 else dd_hbm.at[:, cols(j, cb)]
        return pltpu.make_async_copy(src, dn_slot(ph, j), dn_sem.at[dn_place(ph, j)])

    def start_gu(ph, i):
        gu_copy(ph, 0, i).start()
        gu_copy(ph, 1, i).start()

    loop(0, steps, lambda i: start_gu(0, i))
    loop(0, slots, lambda j: dn_copy(0, j).start())
    loop(0, slots // 2, lambda j: dn_copy(1, j).start())

    for copy in inputs:
        copy.wait()
    gat_b[0, core, :, pl.ds(0, width)] = normed(b_in[...].astype(F32), bg_in[...]).astype(BF16)
    lane = lax.broadcasted_iota(jnp.int32, (rows_b, LANES), 1)
    table = jnp.zeros((rows_b, LANES), F32)
    for k in range(ids_in.shape[1]):
        table = table + jnp.where(ids_in[:, k : k + 1] == lane, rw_in[:, k : k + 1], 0.0)
    high = table.astype(BF16)
    gat_b[0, core, :, pl.ds(width, LANES)] = high
    gat_b[0, core, :, pl.ds(width + LANES, LANES)] = (table - high.astype(F32)).astype(BF16)
    gat_a[0, core] = normed(a_in[...].astype(F32), ag_in[...]).astype(BF16)

    pl.semaphore_wait(barrier, outer + inner - 1)

    def remote(src, dst, send, recv, target):
        return pltpu.make_async_remote_copy(
            src_ref=src, dst_ref=dst, send_sem=send, recv_sem=recv,
            device_id=target, device_id_type=MESH,
        )

    spans = (pl.ds(0, front), pl.ds(front, wide - front))

    def block(t, s):
        if t < 2:
            return gat_b.at[s, core, :, spans[t]]
        return gat_a.at[s, core]

    def z_copy(t, d):
        return remote(
            block(t, 0), block(t, d * inner), gz_send.at[t], gz_recv.at[t, d], line(-d)
        )

    def y_copy(t, d, e):
        s = d * inner
        return remote(
            block(t, s), block(t, s + e), gy_send.at[t], gy_recv.at[t, s + e], cross(-e)
        )

    def c_copy(t, s):
        own = block(t, s)
        return remote(own, own, gc_send.at[t], gc_recv.at[t], sibling)

    flip = p * 2 >= outer

    def turn(i):
        return jnp.where(flip, outer - i, i)

    def start_line(t):
        loop(1, outer, lambda i: z_copy(t, turn(i)).start())

    def start_own(t):
        loop(1, inner, lambda e: y_copy(t, 0, e).start())
        c_copy(t, 0).start()

    def forward_line(t, low=1, high=outer):
        def go(i):
            d = turn(i)
            z_copy(t, d).wait_recv()
            loop(1, inner, lambda e: y_copy(t, d, e).start())
            c_copy(t, d * inner).start()

        loop(low, high, go)

    def forward_cross(t):
        def go(d):
            def arrived(e):
                y_copy(t, d, e).wait_recv()
                c_copy(t, d * inner + e).start()

            loop(1, inner, arrived)

        loop(0, outer, go)

    def gathered(t):
        if t < 2:
            drain(gat_b.at[:, 1 - core, :, spans[t]], gc_recv.at[t])
        else:
            drain(gat_a.at[:, 1 - core], gc_recv.at[t])

    def rows_of(ph, where):
        buf = (gat_b, gat_a)[ph]
        pieces = [buf[s, c, :, where].astype(F32) for c in range(2) for s in range(chips)]
        return jnp.concatenate(pieces, axis=0)

    def hidden(ph, after):
        used = (es, fd)[ph]
        total = n * (rows_b, rows_a)[ph]
        ga = g_acc.at[pl.ds(0, total), pl.ds(0, used)]
        ua = u_acc.at[pl.ds(0, total), pl.ds(0, used)]
        ga[...] = jnp.zeros(ga.shape, F32)
        ua[...] = jnp.zeros(ua.shape, F32)

        def step(i):
            gu_copy(ph, 0, i).wait()
            gu_copy(ph, 1, i).wait()

            def product(c, gate, up):
                x = rows_of(ph, cols(i * (kq // kc) + c, kc)).astype(BF16)
                at = pl.ds(c * kc, kc) if isinstance(c, int) else cols(c, kc)
                one = jnp.dot(x, gu_slot(ph, 0, i)[at, :], preferred_element_type=F32)
                two = jnp.dot(x, gu_slot(ph, 1, i)[at, :], preferred_element_type=F32)
                return (one, two) if gate is None else (gate + one, up + two)

            if total > 64:
                def small(c):
                    ga[...], ua[...] = product(c, ga[...], ua[...])

                loop(0, kq // kc, small)
            else:
                gate = up = None
                for c in range(kq // kc):
                    gate, up = product(c, gate, up)
                ga[...] += gate
                ua[...] += up
            after(i)

        loop(0, steps, step)
        g = ga[...]
        return (g / (1.0 + jnp.exp(-g)) * ua[...]).astype(BF16)

    def tools(ph):
        mine, s1, r1, keep, ys, yr, own, zs, zr = (back_b, back_a)[ph]
        rows = own.shape[0]
        out = (b_out, a_out)[ph]

        def pair_copy(j):
            where = cols(j, cw)
            return remote(
                s1.at[:, where], r1.at[:, where], s1_send.at[ph], s1_recv.at[ph, j], sibling
            )

        def y_send(j, e):
            where = cols(j, cw)
            return remote(
                ys.at[e - 1, :, :, where], yr.at[e - 1, :, :, where],
                s2_send.at[ph], s2_recv.at[ph, j], cross(e),
            )

        def z_send(j, d):
            where = cols(j, cw)
            return remote(
                zs.at[d - 1, :, where], zr.at[d - 1, :, where],
                s3_send.at[ph], s3_recv.at[ph, j], line(d),
            )

        def pair_done(j):
            where = cols(j, cw)
            pair_copy(j).wait_recv()
            both = mine[:, where] + r1[:, where].astype(F32)
            for d in range(outer):
                at = d * inner * rows
                keep[d, :, where] = both[at : at + rows]
                for e in range(1, inner):
                    ys[e - 1, d, :, where] = both[at + e * rows : at + (e + 1) * rows].astype(BF16)
            loop(1, inner, lambda e: y_send(j, e).start())

        def cross_done(j):
            where = cols(j, cw)
            drain(yr.at[:, :, :, where], s2_recv.at[ph, j])
            for d in range(outer):
                total = keep[d, :, where]
                for e in range(1, inner):
                    total = total + yr[e - 1, d, :, where].astype(F32)
                if d:
                    zs[d - 1, :, where] = total.astype(BF16)
                else:
                    own[:, where] = total
            loop(1, outer, lambda d: z_send(j, d).start())

        def line_done(j):
            where = cols(j, cw)
            drain(zr.at[:, :, where], s3_recv.at[ph, j])
            total = own[:, where]
            for d in range(1, outer):
                total = total + zr[d - 1, :, where].astype(F32)
            out[:, where] = total

        def down(low, high):
            hid = (hid_b, hid_a)[ph]
            loop(low, high, lambda j: dn_copy(ph, j).wait())

            def one(j):
                value = jnp.dot(hid[...], dn_slot(ph, j)[...], preferred_element_type=F32)
                if ph == 0:
                    value = value * scale
                count = mine.shape[0]
                first, second = value[:count], value[count:]
                at = cols(j, cb)
                mine[:, at] = jnp.where(core == 0, first, second)
                s1[:, at] = jnp.where(core == 0, second, first).astype(BF16)

            if n > 32:
                loop(low, high, one)
            else:
                for j in range(low, high):
                    one(j)
            loop(low * cb // cw, high * cb // cw, lambda j: pair_copy(j).start())

        return down, pair_done, cross_done, line_done

    down_b, pair_done_b, cross_done_b, line_done_b = tools(0)
    down_a, pair_done_a, cross_done_a, line_done_a = tools(1)
    mid = chunks // 2

    start_line(0)
    start_own(0)
    forward_line(0, 1, 2)
    start_line(1)
    forward_line(0, 2, outer)
    start_own(1)
    start_line(2)
    forward_cross(0)
    forward_line(1)
    gathered(0)

    def after_b(i):
        start_gu(1, i)

        @pl.when(i == 0)
        def _():
            forward_cross(1)
            start_own(2)
            forward_line(2)

        @pl.when(i == steps // 2 - 1)
        def _():
            gathered(1)

        @pl.when(i == steps // 2)
        def _():
            forward_cross(2)

    hid_b[...] = hidden(0, after_b)
    tables = rows_of(0, pl.ds(width, LANES)) + rows_of(0, pl.ds(width + LANES, LANES))
    chosen = lax.broadcasted_iota(jnp.int32, tables.shape, 1) == expert
    scale = jnp.sum(jnp.where(chosen, tables, 0.0), axis=1, keepdims=True)
    down_b(0, slots // 2)
    loop(slots // 2, slots, lambda j: dn_copy(1, j).start())
    gathered(2)

    def after_a(i):
        @pl.when(i == 0)
        def _():
            loop(0, chunks, pair_done_b)

        @pl.when(i == steps - 1)
        def _():
            loop(0, mid, cross_done_b)

    down_b(slots // 2, slots)
    hid_a[...] = hidden(1, after_a)
    down_a(0, mid)
    loop(mid, chunks - 1, cross_done_b)
    down_a(mid, chunks - 1)
    loop(0, mid, pair_done_a)
    loop(chunks - 1, chunks, cross_done_b)
    down_a(chunks - 1, chunks)
    loop(mid, chunks - 1, pair_done_a)
    loop(0, mid, line_done_b)
    loop(chunks - 1, chunks, pair_done_a)
    loop(0, mid, cross_done_a)
    loop(mid, chunks, line_done_b)
    loop(mid, chunks, cross_done_a)
    loop(0, chunks, line_done_a)

    for t in range(3):
        def sent(count):
            if t < 2:
                return gat_b.at[pl.ds(0, count), 0, :, spans[t]]
            return gat_a.at[pl.ds(0, count), 0]

        drain(sent(outer - 1), gz_send.at[t])
        drain(sent(outer * (inner - 1)), gy_send.at[t])
        drain(sent(chips), gc_send.at[t])
    for ph in range(2):
        s1, ys, zs = (back_b, back_a)[ph][1], (back_b, back_a)[ph][4], (back_b, back_a)[ph][7]
        drain(s1, s1_send.at[ph])
        drain(ys, s2_send.at[ph])
        drain(zs, s3_send.at[ph])


def finish(sum_a, sum_b, a_ref, b_ref, a_out, b_out):
    a_out[...] = (a_ref[...].astype(F32) + sum_a[...]).astype(BF16)
    b_out[...] = (b_ref[...].astype(F32) + sum_b[...]).astype(BF16)


def shards(
    a_tokens, a_gain, dense_gate, dense_up, dense_down, b_tokens, b_gain, expert_ids,
    route_weights, expert_gate, expert_up, expert_down,
):
    n = lax.axis_size("exp")
    chips = n // 2
    outer, inner = factor(chips)
    ra, width = a_tokens.shape
    rb = b_tokens.shape[0]
    fd = dense_gate.shape[1]
    es = expert_gate.shape[2]
    kq = width // 4
    kc = pick(kq, (256, 128))
    cb = cw = width // 4
    steps, slots = width // kq, width // cb
    extra_width = width + 2 * LANES
    most = n * max(ra, rb)

    def back(rows, span):
        return [
            pltpu.VMEM((chips * rows, span), F32),
            pltpu.VMEM((chips * rows, span), BF16),
            pltpu.VMEM((chips * rows, span), BF16),
            pltpu.VMEM((outer, rows, span), F32),
            pltpu.VMEM((inner - 1, outer, rows, span), BF16),
            pltpu.VMEM((inner - 1, outer, rows, span), BF16),
            pltpu.VMEM((rows, span), F32),
            pltpu.VMEM((outer - 1, rows, span), BF16),
            pltpu.VMEM((outer - 1, rows, span), BF16),
        ]

    vmem = pl.BlockSpec(memory_space=pltpu.VMEM)
    hbm = pl.BlockSpec(memory_space=pl.ANY)
    dma = pltpu.SemaphoreType.DMA
    weights = 3 * width * (fd + es)
    gains = (a_gain.reshape(1, width), b_gain.reshape(1, width))
    sums = pl.pallas_call(
        functools.partial(kernel, n, kq, kc, cb, cw),
        out_shape=(
            jax.ShapeDtypeStruct(a_tokens.shape, F32),
            jax.ShapeDtypeStruct(b_tokens.shape, F32),
        ),
        in_specs=[hbm] * 12,
        out_specs=(vmem, vmem),
        scratch_shapes=[
            pltpu.VMEM(a_tokens.shape, BF16),
            pltpu.VMEM((1, width), F32),
            pltpu.VMEM(b_tokens.shape, BF16),
            pltpu.VMEM((1, width), F32),
            pltpu.VMEM(expert_ids.shape, jnp.int32),
            pltpu.VMEM(route_weights.shape, F32),
            pltpu.VMEM((2, steps, kq, max(fd, es)), BF16),
            pltpu.VMEM((slots + slots // 2, max(fd, es), cb), BF16),
            pltpu.VMEM((chips, 2, rb, extra_width), BF16),
            pltpu.VMEM((chips, 2, ra, width), BF16),
            pltpu.VMEM((most, max(fd, es)), F32),
            pltpu.VMEM((most, max(fd, es)), F32),
            pltpu.VMEM((n * rb, es), BF16),
            pltpu.VMEM((n * ra, fd), BF16),
            back(rb, width),
            back(ra, width),
            dma((6,)),
            dma((2, steps)),
            dma((slots + slots // 2,)),
            dma((3,)),
            dma((3, outer)),
            dma((3,)),
            dma((3, chips)),
            dma((3,)),
            dma((3,)),
            dma((2,)),
            dma((2, width // cw)),
            dma((2,)),
            dma((2, width // cw)),
            dma((2,)),
            dma((2, width // cw)),
        ],
        compiler_params=pltpu.CompilerParams(
            collective_id=0, has_side_effects=True, vmem_limit_bytes=67043328
        ),
        cost_estimate=pl.CostEstimate(
            flops=2 * n * max(ra, rb) * weights, bytes_accessed=2 * weights, transcendentals=0
        ),
    )(
        a_tokens, gains[0], b_tokens, gains[1], expert_ids, route_weights,
        dense_gate, dense_up, dense_down, expert_gate, expert_up, expert_down,
    )
    return pl.pallas_call(
        finish,
        out_shape=(
            jax.ShapeDtypeStruct(a_tokens.shape, BF16),
            jax.ShapeDtypeStruct(b_tokens.shape, BF16),
        ),
        in_specs=[vmem] * 4,
        out_specs=(vmem, vmem),
    )(*sums, a_tokens, b_tokens)


def solution(mesh):
    return jax.shard_map(
        shards,
        mesh=mesh,
        in_specs=(
            P(("rep", "exp"), None),
            P(),
            P(None, "exp"),
            P(None, "exp"),
            P("exp", None),
            P(("rep", "exp"), None),
            P(),
            P(("rep", "exp"), None),
            P(("rep", "exp"), None),
            P("exp", None, None),
            P("exp", None, None),
            P("exp", None, None),
        ),
        out_specs=(P(("rep", "exp"), None), P(("rep", "exp"), None)),
        check_vma=False,
    )
```

```python
import functools

import jax
import jax.numpy as jnp
from jax import lax
from jax.experimental import pallas as pl
from jax.experimental.pallas import tpu as pltpu
from jax.sharding import PartitionSpec as P

EXPERTS = 16
LANES = 128
F32 = jnp.float32
BF16 = jnp.bfloat16
MESH = pl.DeviceIdType.MESH


def pick(total, sizes):
    for size in sizes:
        if total % size == 0:
            return size
    return total


def factor(chips):
    inner = 1
    while inner * inner * 4 <= chips and chips % (inner * 2) == 0:
        inner *= 2
    return chips // inner, inner


def normed(values, gain_row):
    mean = jnp.mean(values * values, axis=-1, keepdims=True)
    return values * lax.rsqrt(mean + 1e-06) * gain_row


def drain(ref, sem):
    pltpu.make_async_copy(ref, ref, sem).wait()


def kernel(
    n, kq, kc, cb, cw,
    a_hbm, ag_hbm, b_hbm, bg_hbm, ids_hbm, rw_hbm,
    dg_hbm, du_hbm, dd_hbm, eg_hbm, eu_hbm, ed_hbm,
    a_out, b_out,
    a_in, ag_in, b_in, bg_in, ids_in, rw_in,
    gu, dn, gat_b, gat_a, g_acc, u_acc, hid_b, hid_a,
    back_b, back_a,
    in_sem, gu_sem, dn_sem,
    gz_send, gz_recv, gy_send, gy_recv, gc_send, gc_recv,
    s1_send, s1_recv, s2_send, s2_recv, s3_send, s3_recv,
):
    me = lax.axis_index("exp")
    core = lax.rem(me, 2)
    chip = me // 2
    chips = n // 2
    outer, inner = factor(chips)
    p = chip // inner
    q = lax.rem(chip, inner)
    expert = me // (n // EXPERTS)
    rows_a, width = a_in.shape
    rows_b = b_in.shape[0]
    steps = width // kq
    slots = width // cb
    chunks = width // cw
    es = eg_hbm.shape[2]
    fd = dg_hbm.shape[1]
    front = width // 2
    wide = gat_b.shape[3]
    sibling = {"exp": chip * 2 + (1 - core)}

    def line(d):
        return {"exp": (lax.rem(p + d + outer, outer) * inner + q) * 2 + core}

    def cross(e):
        return {"exp": (p * inner + lax.rem(q + e + inner, inner)) * 2 + core}

    def cols(j, size):
        return pl.ds(pl.multiple_of(j * size, size), size)

    def loop(low, high, body):
        def go(i, carry):
            body(i)
            return carry

        lax.fori_loop(low, high, go, 0)

    def signal(target):
        pl.semaphore_signal(barrier, inc=1, device_id=target, device_id_type=MESH)

    barrier = pltpu.get_barrier_semaphore()
    loop(1, outer, lambda d: signal(line(d)))
    loop(1, inner, lambda e: signal(cross(e)))
    signal(sibling)

    inputs = [
        pltpu.make_async_copy(src, dst, in_sem.at[i])
        for i, (src, dst) in enumerate((
            (b_hbm, b_in), (bg_hbm, bg_in), (ids_hbm, ids_in),
            (rw_hbm, rw_in), (a_hbm, a_in), (ag_hbm, ag_in),
        ))
    ]
    for copy in inputs:
        copy.start()

    def gu_slot(ph, w, i):
        return gu.at[w, i, :, pl.ds(0, (es, fd)[ph])]

    def gu_copy(ph, w, i):
        if ph == 0:
            src = (eg_hbm, eu_hbm)[w].at[0, cols(i, kq), :]
        else:
            src = (dg_hbm, du_hbm)[w].at[cols(i, kq), :]
        return pltpu.make_async_copy(src, gu_slot(ph, w, i), gu_sem.at[w, i])

    def dn_place(ph, j):
        return j if ph == 0 else (j + slots) % (slots + slots // 2)

    def dn_slot(ph, j):
        return dn.at[dn_place(ph, j), pl.ds(0, (es, fd)[ph])]

    def dn_copy(ph, j):
        src = ed_hbm.at[0, :, cols(j, cb)] if ph == 0 else dd_hbm.at[:, cols(j, cb)]
        return pltpu.make_async_copy(src, dn_slot(ph, j), dn_sem.at[dn_place(ph, j)])

    def start_gu(ph, i):
        gu_copy(ph, 0, i).start()
        gu_copy(ph, 1, i).start()

    loop(0, steps, lambda i: start_gu(0, i))
    loop(0, slots, lambda j: dn_copy(0, j).start())
    loop(0, slots // 2, lambda j: dn_copy(1, j).start())

    for copy in inputs:
        copy.wait()
    gat_b[0, core, :, pl.ds(0, width)] = normed(b_in[...].astype(F32), bg_in[...]).astype(BF16)
    lane = lax.broadcasted_iota(jnp.int32, (rows_b, LANES), 1)
    table = jnp.zeros((rows_b, LANES), F32)
    for k in range(ids_in.shape[1]):
        table = table + jnp.where(ids_in[:, k : k + 1] == lane, rw_in[:, k : k + 1], 0.0)
    high = table.astype(BF16)
    gat_b[0, core, :, pl.ds(width, LANES)] = high
    gat_b[0, core, :, pl.ds(width + LANES, LANES)] = (table - high.astype(F32)).astype(BF16)
    gat_a[0, core] = normed(a_in[...].astype(F32), ag_in[...]).astype(BF16)

    pl.semaphore_wait(barrier, outer + inner - 1)

    def remote(src, dst, send, recv, target):
        return pltpu.make_async_remote_copy(
            src_ref=src, dst_ref=dst, send_sem=send, recv_sem=recv,
            device_id=target, device_id_type=MESH,
        )

    spans = (pl.ds(0, front), pl.ds(front, wide - front))

    def block(t, s):
        if t < 2:
            return gat_b.at[s, core, :, spans[t]]
        return gat_a.at[s, core]

    def z_copy(t, d):
        return remote(
            block(t, 0), block(t, d * inner), gz_send.at[t], gz_recv.at[t, d], line(-d)
        )

    def y_copy(t, d, e):
        s = d * inner
        return remote(
            block(t, s), block(t, s + e), gy_send.at[t], gy_recv.at[t, s + e], cross(-e)
        )

    def c_copy(t, s):
        own = block(t, s)
        return remote(own, own, gc_send.at[t], gc_recv.at[t], sibling)

    flip = p * 2 >= outer

    def turn(i):
        return jnp.where(flip, outer - i, i)

    def start_line(t):
        loop(1, outer, lambda i: z_copy(t, turn(i)).start())

    def start_own(t):
        loop(1, inner, lambda e: y_copy(t, 0, e).start())
        c_copy(t, 0).start()

    def forward_line(t, low=1, high=outer):
        def go(i):
            d = turn(i)
            z_copy(t, d).wait_recv()
            loop(1, inner, lambda e: y_copy(t, d, e).start())
            c_copy(t, d * inner).start()

        loop(low, high, go)

    def forward_cross(t):
        def go(d):
            def arrived(e):
                y_copy(t, d, e).wait_recv()
                c_copy(t, d * inner + e).start()

            loop(1, inner, arrived)

        loop(0, outer, go)

    def gathered(t):
        if t < 2:
            drain(gat_b.at[:, 1 - core, :, spans[t]], gc_recv.at[t])
        else:
            drain(gat_a.at[:, 1 - core], gc_recv.at[t])

    def rows_of(ph, where):
        buf = (gat_b, gat_a)[ph]
        pieces = [buf[s, c, :, where].astype(F32) for c in range(2) for s in range(chips)]
        return jnp.concatenate(pieces, axis=0)

    def hidden(ph, after):
        used = (es, fd)[ph]
        total = n * (rows_b, rows_a)[ph]
        ga = g_acc.at[pl.ds(0, total), pl.ds(0, used)]
        ua = u_acc.at[pl.ds(0, total), pl.ds(0, used)]
        ga[...] = jnp.zeros(ga.shape, F32)
        ua[...] = jnp.zeros(ua.shape, F32)

        span = (2, 1)[ph]

        def step(i):
            for k in range(span):
                gu_copy(ph, 0, i * span + k).wait()
                gu_copy(ph, 1, i * span + k).wait()

            def product(k, c, gate, up):
                at = i * span + k
                x = rows_of(ph, cols(at * (kq // kc) + c, kc)).astype(BF16)
                rows = pl.ds(c * kc, kc) if isinstance(c, int) else cols(c, kc)
                one = jnp.dot(x, gu_slot(ph, 0, at)[rows, :], preferred_element_type=F32)
                two = jnp.dot(x, gu_slot(ph, 1, at)[rows, :], preferred_element_type=F32)
                return (one, two) if gate is None else (gate + one, up + two)

            if total > 64:
                for k in range(span):
                    def small(c, k=k):
                        ga[...], ua[...] = product(k, c, ga[...], ua[...])

                    loop(0, kq // kc, small)
            else:
                gate = up = None
                for k in range(span):
                    for c in range(kq // kc):
                        gate, up = product(k, c, gate, up)
                ga[...] += gate
                ua[...] += up
            after(i)

        loop(0, steps // span, step)
        g = ga[...]
        return (g / (1.0 + jnp.exp(-g)) * ua[...]).astype(BF16)

    def tools(ph):
        mine, s1, r1, keep, ys, yr, own, zs, zr = (back_b, back_a)[ph]
        rows = own.shape[0]
        out, tokens = ((b_out, b_in), (a_out, a_in))[ph]

        def pair_copy(j):
            where = cols(j, cw)
            return remote(
                s1.at[:, where], r1.at[:, where], s1_send.at[ph], s1_recv.at[ph, j], sibling
            )

        def y_send(j, e):
            where = cols(j, cw)
            return remote(
                ys.at[e - 1, :, :, where], yr.at[e - 1, :, :, where],
                s2_send.at[ph], s2_recv.at[ph, j], cross(e),
            )

        def z_send(j, d):
            where = cols(j, cw)
            return remote(
                zs.at[d - 1, :, where], zr.at[d - 1, :, where],
                s3_send.at[ph], s3_recv.at[ph, j], line(d),
            )

        def pair_done(j):
            where = cols(j, cw)
            pair_copy(j).wait_recv()
            both = mine[:, where] + r1[:, where].astype(F32)
            for d in range(outer):
                at = d * inner * rows
                keep[d, :, where] = both[at : at + rows]
                for e in range(1, inner):
                    ys[e - 1, d, :, where] = both[at + e * rows : at + (e + 1) * rows].astype(BF16)
            loop(1, inner, lambda e: y_send(j, e).start())

        def cross_done(j):
            where = cols(j, cw)
            drain(yr.at[:, :, :, where], s2_recv.at[ph, j])
            for d in range(outer):
                total = keep[d, :, where]
                for e in range(1, inner):
                    total = total + yr[e - 1, d, :, where].astype(F32)
                if d:
                    zs[d - 1, :, where] = total.astype(BF16)
                else:
                    own[:, where] = total
            loop(1, outer, lambda d: z_send(j, d).start())

        def line_done(j):
            where = cols(j, cw)
            drain(zr.at[:, :, where], s3_recv.at[ph, j])
            total = own[:, where]
            for d in range(1, outer):
                total = total + zr[d - 1, :, where].astype(F32)
            out[:, where] = tokens[:, where].astype(F32) + total

        def down(low, high):
            hid = (hid_b, hid_a)[ph]
            loop(low, high, lambda j: dn_copy(ph, j).wait())

            def one(j):
                value = jnp.dot(hid[...], dn_slot(ph, j)[...], preferred_element_type=F32)
                if ph == 0:
                    value = value * scale
                count = mine.shape[0]
                first, second = value[:count], value[count:]
                at = cols(j, cb)
                mine[:, at] = jnp.where(core == 0, first, second)
                s1[:, at] = jnp.where(core == 0, second, first).astype(BF16)

            if n > 32:
                loop(low, high, one)
            else:
                for j in range(low, high):
                    one(j)
            loop(low * cb // cw, high * cb // cw, lambda j: pair_copy(j).start())

        return down, pair_done, cross_done, line_done

    down_b, pair_done_b, cross_done_b, line_done_b = tools(0)
    down_a, pair_done_a, cross_done_a, line_done_a = tools(1)
    mid = chunks // 2

    start_line(0)
    start_own(0)
    forward_line(0, 1, 2)
    start_line(1)
    forward_line(0, 2, outer)
    start_own(1)
    start_line(2)
    forward_cross(0)
    forward_line(1)
    gathered(0)

    def after_b(i):
        start_gu(1, 2 * i)
        start_gu(1, 2 * i + 1)

        @pl.when(i == 0)
        def _():
            forward_cross(1)
            start_own(2)
            forward_line(2)
            gathered(1)

        @pl.when(i == 1)
        def _():
            forward_cross(2)

    hid_b[...] = hidden(0, after_b)
    tables = rows_of(0, pl.ds(width, LANES)) + rows_of(0, pl.ds(width + LANES, LANES))
    chosen = lax.broadcasted_iota(jnp.int32, tables.shape, 1) == expert
    scale = jnp.sum(jnp.where(chosen, tables, 0.0), axis=1, keepdims=True)
    down_b(0, slots // 2)
    loop(slots // 2, slots, lambda j: dn_copy(1, j).start())
    gathered(2)

    def after_a(i):
        @pl.when(i == 0)
        def _():
            loop(mid, chunks, pair_done_b)

        @pl.when(i == steps - 2)
        def _():
            loop(0, mid, cross_done_b)

    down_b(slots // 2, slots)
    loop(0, mid, pair_done_b)
    hid_a[...] = hidden(1, after_a)
    down_a(0, mid)
    loop(mid, chunks - 1, cross_done_b)
    down_a(mid, chunks - 1)
    loop(0, mid, pair_done_a)
    loop(chunks - 1, chunks, cross_done_b)
    down_a(chunks - 1, chunks)
    loop(mid, chunks - 1, pair_done_a)
    loop(0, mid, line_done_b)
    loop(chunks - 1, chunks, pair_done_a)
    loop(0, mid, cross_done_a)
    loop(mid, chunks, line_done_b)
    loop(mid, chunks, cross_done_a)
    loop(0, chunks, line_done_a)

    for t in range(3):
        def sent(count):
            if t < 2:
                return gat_b.at[pl.ds(0, count), 0, :, spans[t]]
            return gat_a.at[pl.ds(0, count), 0]

        drain(sent(outer - 1), gz_send.at[t])
        drain(sent(outer * (inner - 1)), gy_send.at[t])
        drain(sent(chips), gc_send.at[t])
    for ph in range(2):
        s1, ys, zs = (back_b, back_a)[ph][1], (back_b, back_a)[ph][4], (back_b, back_a)[ph][7]
        drain(s1, s1_send.at[ph])
        drain(ys, s2_send.at[ph])
        drain(zs, s3_send.at[ph])


def finish(sum_a, sum_b, a_out, b_out):
    a_out[...] = sum_a[...].astype(BF16)
    b_out[...] = sum_b[...].astype(BF16)


def shards(
    a_tokens, a_gain, dense_gate, dense_up, dense_down, b_tokens, b_gain, expert_ids,
    route_weights, expert_gate, expert_up, expert_down,
):
    n = lax.axis_size("exp")
    chips = n // 2
    outer, inner = factor(chips)
    ra, width = a_tokens.shape
    rb = b_tokens.shape[0]
    fd = dense_gate.shape[1]
    es = expert_gate.shape[2]
    kq = width // 4
    kc = pick(kq, (256, 128))
    cb = cw = width // 4
    steps, slots = width // kq, width // cb
    extra_width = width + 2 * LANES
    most = n * max(ra, rb)

    def back(rows, span):
        return [
            pltpu.VMEM((chips * rows, span), F32),
            pltpu.VMEM((chips * rows, span), BF16),
            pltpu.VMEM((chips * rows, span), BF16),
            pltpu.VMEM((outer, rows, span), F32),
            pltpu.VMEM((inner - 1, outer, rows, span), BF16),
            pltpu.VMEM((inner - 1, outer, rows, span), BF16),
            pltpu.VMEM((rows, span), F32),
            pltpu.VMEM((outer - 1, rows, span), BF16),
            pltpu.VMEM((outer - 1, rows, span), BF16),
        ]

    vmem = pl.BlockSpec(memory_space=pltpu.VMEM)
    hbm = pl.BlockSpec(memory_space=pl.ANY)
    dma = pltpu.SemaphoreType.DMA
    weights = 3 * width * (fd + es)
    gains = (a_gain.reshape(1, width), b_gain.reshape(1, width))
    sums = pl.pallas_call(
        functools.partial(kernel, n, kq, kc, cb, cw),
        out_shape=(
            pltpu.VMEM(a_tokens.shape, F32),
            pltpu.VMEM(b_tokens.shape, F32),
        ),
        in_specs=[hbm] * 12,
        out_specs=(vmem, vmem),
        scratch_shapes=[
            pltpu.VMEM(a_tokens.shape, BF16),
            pltpu.VMEM((1, width), F32),
            pltpu.VMEM(b_tokens.shape, BF16),
            pltpu.VMEM((1, width), F32),
            pltpu.VMEM(expert_ids.shape, jnp.int32),
            pltpu.VMEM(route_weights.shape, F32),
            pltpu.VMEM((2, steps, kq, max(fd, es)), BF16),
            pltpu.VMEM((slots + slots // 2, max(fd, es), cb), BF16),
            pltpu.VMEM((chips, 2, rb, extra_width), BF16),
            pltpu.VMEM((chips, 2, ra, width), BF16),
            pltpu.VMEM((most, max(fd, es)), F32),
            pltpu.VMEM((most, max(fd, es)), F32),
            pltpu.VMEM((n * rb, es), BF16),
            pltpu.VMEM((n * ra, fd), BF16),
            back(rb, width),
            back(ra, width),
            dma((6,)),
            dma((2, steps)),
            dma((slots + slots // 2,)),
            dma((3,)),
            dma((3, outer)),
            dma((3,)),
            dma((3, chips)),
            dma((3,)),
            dma((3,)),
            dma((2,)),
            dma((2, width // cw)),
            dma((2,)),
            dma((2, width // cw)),
            dma((2,)),
            dma((2, width // cw)),
        ],
        compiler_params=pltpu.CompilerParams(
            collective_id=0, has_side_effects=True, vmem_limit_bytes=66400000
        ),
        cost_estimate=pl.CostEstimate(
            flops=2 * n * max(ra, rb) * weights, bytes_accessed=2 * weights, transcendentals=0
        ),
    )(
        a_tokens, gains[0], b_tokens, gains[1], expert_ids, route_weights,
        dense_gate, dense_up, dense_down, expert_gate, expert_up, expert_down,
    )
    return pl.pallas_call(
        finish,
        out_shape=(
            jax.ShapeDtypeStruct(a_tokens.shape, BF16),
            jax.ShapeDtypeStruct(b_tokens.shape, BF16),
        ),
        in_specs=[vmem] * 2,
        out_specs=(vmem, vmem),
    )(*[pltpu.with_memory_space_constraint(x, pltpu.VMEM) for x in sums])


def solution(mesh):
    return jax.shard_map(
        shards,
        mesh=mesh,
        in_specs=(
            P(("rep", "exp"), None),
            P(),
            P(None, "exp"),
            P(None, "exp"),
            P("exp", None),
            P(("rep", "exp"), None),
            P(),
            P(("rep", "exp"), None),
            P(("rep", "exp"), None),
            P("exp", None, None),
            P("exp", None, None),
            P("exp", None, None),
        ),
        out_specs=(P(("rep", "exp"), None), P(("rep", "exp"), None)),
        check_vma=False,
    )
```

```python
import functools

import jax
import jax.numpy as jnp
from jax import lax
from jax.experimental import pallas as pl
from jax.experimental.pallas import tpu as pltpu
from jax.sharding import PartitionSpec as P

EXPERTS = 16
LANES = 128
F32 = jnp.float32
BF16 = jnp.bfloat16
MESH = pl.DeviceIdType.MESH
FAR = 3


def pick(total, sizes):
    for size in sizes:
        if total % size == 0:
            return size
    return total


def factor(chips):
    inner = 1
    while inner * inner * 4 <= chips and chips % (inner * 2) == 0:
        inner *= 2
    return chips // inner, inner


def normed(values, gain_row):
    mean = jnp.mean(values * values, axis=-1, keepdims=True)
    return values * lax.rsqrt(mean + 1e-06) * gain_row


def drain(ref, sem):
    pltpu.make_async_copy(ref, ref, sem).wait()


def kernel(
    n, kq, kc, cb, cw,
    a_hbm, ag_hbm, b_hbm, bg_hbm, ids_hbm, rw_hbm,
    dg_hbm, du_hbm, dd_hbm, eg_hbm, eu_hbm, ed_hbm,
    a_out, b_out,
    a_in, ag_in, b_in, bg_in, ids_in, rw_in,
    gu, dn, gat_b, gat_a, g_acc, u_acc, hid_b, hid_a,
    back_b, back_a, far_out, far_in,
    in_sem, gu_sem, dn_sem,
    gz_send, gz_recv, gy_send, gy_recv, gc_send, gc_recv,
    s1_send, s1_recv, s2_send, s2_recv, s3_send, s3_recv, far_send, far_recv,
):
    me = lax.axis_index("exp")
    core = lax.rem(me, 2)
    chip = me // 2
    chips = n // 2
    outer, inner = factor(chips)
    p = chip // inner
    q = lax.rem(chip, inner)
    expert = me // (n // EXPERTS)
    rows_a, width = a_in.shape
    rows_b = b_in.shape[0]
    steps = width // kq
    slots = width // cb
    chunks = width // cw
    es = eg_hbm.shape[2]
    fd = dg_hbm.shape[1]
    front = width // 2
    wide = gat_b.shape[3]
    sibling = {"exp": chip * 2 + (1 - core)}

    def line(d):
        return {"exp": (lax.rem(p + d + outer, outer) * inner + q) * 2 + core}

    def cross(e):
        return {"exp": (p * inner + lax.rem(q + e + inner, inner)) * 2 + core}

    def cols(j, size):
        return pl.ds(pl.multiple_of(j * size, size), size)

    def loop(low, high, body):
        def go(i, carry):
            body(i)
            return carry

        lax.fori_loop(low, high, go, 0)

    def signal(target):
        pl.semaphore_signal(barrier, inc=1, device_id=target, device_id_type=MESH)

    barrier = pltpu.get_barrier_semaphore()
    loop(1, outer, lambda d: signal(line(d)))
    loop(1, inner, lambda e: signal(cross(e)))
    signal(sibling)

    inputs = [
        pltpu.make_async_copy(src, dst, in_sem.at[i])
        for i, (src, dst) in enumerate((
            (b_hbm, b_in), (bg_hbm, bg_in), (ids_hbm, ids_in),
            (rw_hbm, rw_in), (a_hbm, a_in), (ag_hbm, ag_in),
        ))
    ]
    for copy in inputs:
        copy.start()

    def gu_slot(ph, w, i):
        return gu.at[w, i, :, pl.ds(0, (es, fd)[ph])]

    def gu_copy(ph, w, i):
        if ph == 0:
            src = (eg_hbm, eu_hbm)[w].at[0, cols(i, kq), :]
        else:
            src = (dg_hbm, du_hbm)[w].at[cols(i, kq), :]
        return pltpu.make_async_copy(src, gu_slot(ph, w, i), gu_sem.at[w, i])

    def dn_place(ph, j):
        return j if ph == 0 else (j + slots) % (slots + slots // 2)

    def dn_slot(ph, j):
        return dn.at[dn_place(ph, j), pl.ds(0, (es, fd)[ph])]

    def dn_copy(ph, j):
        src = ed_hbm.at[0, :, cols(j, cb)] if ph == 0 else dd_hbm.at[:, cols(j, cb)]
        return pltpu.make_async_copy(src, dn_slot(ph, j), dn_sem.at[dn_place(ph, j)])

    def start_gu(ph, i):
        gu_copy(ph, 0, i).start()
        gu_copy(ph, 1, i).start()

    loop(0, steps, lambda i: start_gu(0, i))
    loop(0, slots, lambda j: dn_copy(0, j).start())
    loop(0, slots // 2, lambda j: dn_copy(1, j).start())

    for copy in inputs[:4]:
        copy.wait()
    gat_b[0, core, :, pl.ds(0, width)] = normed(b_in[...].astype(F32), bg_in[...]).astype(BF16)
    lane = lax.broadcasted_iota(jnp.int32, (rows_b, LANES), 1)
    table = jnp.zeros((rows_b, LANES), F32)
    for k in range(ids_in.shape[1]):
        table = table + jnp.where(ids_in[:, k : k + 1] == lane, rw_in[:, k : k + 1], 0.0)
    high = table.astype(BF16)
    gat_b[0, core, :, pl.ds(width, LANES)] = high
    gat_b[0, core, :, pl.ds(width + LANES, LANES)] = (table - high.astype(F32)).astype(BF16)
    pl.semaphore_wait(barrier, outer + inner - 1)

    def remote(src, dst, send, recv, target):
        return pltpu.make_async_remote_copy(
            src_ref=src, dst_ref=dst, send_sem=send, recv_sem=recv,
            device_id=target, device_id_type=MESH,
        )

    spans = (pl.ds(0, front), pl.ds(front, wide - front))

    def block(t, s):
        if t < 2:
            return gat_b.at[s, core, :, spans[t]]
        return gat_a.at[s, core]

    def z_copy(t, d):
        return remote(
            block(t, 0), block(t, d * inner), gz_send.at[t], gz_recv.at[t, d], line(-d)
        )

    def y_copy(t, d, e):
        s = d * inner
        return remote(
            block(t, s), block(t, s + e), gy_send.at[t], gy_recv.at[t, s + e], cross(-e)
        )

    def c_copy(t, s):
        own = block(t, s)
        return remote(own, own, gc_send.at[t], gc_recv.at[t], sibling)

    flip = p * 2 >= outer

    def turn(i):
        return jnp.where(flip, outer - i, i)

    def start_line(t):
        loop(1, outer, lambda i: z_copy(t, turn(i)).start())

    def start_own(t):
        loop(1, inner, lambda e: y_copy(t, 0, e).start())
        c_copy(t, 0).start()

    def forward_line(t, low=1, high=outer):
        def go(i):
            d = turn(i)
            z_copy(t, d).wait_recv()
            loop(1, inner, lambda e: y_copy(t, d, e).start())
            c_copy(t, d * inner).start()

        loop(low, high, go)

    def forward_cross(t):
        def go(d):
            def arrived(e):
                y_copy(t, d, e).wait_recv()
                c_copy(t, d * inner + e).start()

            loop(1, inner, arrived)

        loop(0, outer, go)

    def gathered(t):
        if t < 2:
            drain(gat_b.at[:, 1 - core, :, spans[t]], gc_recv.at[t])
        else:
            drain(gat_a.at[:, 1 - core], gc_recv.at[t])

    def rows_of(ph, where):
        buf = (gat_b, gat_a)[ph]
        pieces = [buf[s, c, :, where].astype(F32) for c in range(2) for s in range(chips)]
        return jnp.concatenate(pieces, axis=0)

    def hidden(ph, after):
        used = (es, fd)[ph]
        total = n * (rows_b, rows_a)[ph]
        ga = g_acc.at[pl.ds(0, total), pl.ds(0, used)]
        ua = u_acc.at[pl.ds(0, total), pl.ds(0, used)]
        ga[...] = jnp.zeros(ga.shape, F32)
        ua[...] = jnp.zeros(ua.shape, F32)

        span = (2, 1)[ph]

        def step(i):
            for k in range(span):
                gu_copy(ph, 0, i * span + k).wait()
                gu_copy(ph, 1, i * span + k).wait()

            def product(k, c, gate, up):
                at = i * span + k
                x = rows_of(ph, cols(at * (kq // kc) + c, kc)).astype(BF16)
                rows = pl.ds(c * kc, kc) if isinstance(c, int) else cols(c, kc)
                one = jnp.dot(x, gu_slot(ph, 0, at)[rows, :], preferred_element_type=F32)
                two = jnp.dot(x, gu_slot(ph, 1, at)[rows, :], preferred_element_type=F32)
                return (one, two) if gate is None else (gate + one, up + two)

            if total > 64:
                for k in range(span):
                    def small(c, k=k):
                        ga[...], ua[...] = product(k, c, ga[...], ua[...])

                    loop(0, kq // kc, small)
            else:
                gate = up = None
                for k in range(span):
                    for c in range(kq // kc):
                        gate, up = product(k, c, gate, up)
                ga[...] += gate
                ua[...] += up
            after(i)

        loop(0, steps // span, step)
        g = ga[...]
        return (g / (1.0 + jnp.exp(-g)) * ua[...]).astype(BF16)

    def tools(ph):
        mine, s1, r1, keep, ys, yr, own, zs, zr = (back_b, back_a)[ph]
        rows = own.shape[0]
        out, tokens = ((b_out, b_in), (a_out, a_in))[ph]

        def pair_copy(j):
            where = cols(j, cw)
            return remote(
                s1.at[:, where], r1.at[:, where], s1_send.at[ph], s1_recv.at[ph, j], sibling
            )

        def y_send(j, e):
            where = cols(j, cw)
            return remote(
                ys.at[e - 1, :, :, where], yr.at[e - 1, :, :, where],
                s2_send.at[ph], s2_recv.at[ph, j], cross(e),
            )

        def z_send(j, d):
            where = cols(j, cw)
            return remote(
                zs.at[d - 1, :, where], zr.at[d - 1, :, where],
                s3_send.at[ph], s3_recv.at[ph, j], line(d),
            )

        def pair_done(j):
            where = cols(j, cw)
            pair_copy(j).wait_recv()
            both = mine[:, where] + r1[:, where].astype(F32)
            for d in range(outer):
                at = d * inner * rows
                keep[d, :, where] = both[at : at + rows]
                for e in range(1, inner):
                    ys[e - 1, d, :, where] = both[at + e * rows : at + (e + 1) * rows].astype(BF16)
            loop(1, inner, lambda e: y_send(j, e).start())

        def cross_done(j):
            where = cols(j, cw)
            drain(yr.at[:, :, :, where], s2_recv.at[ph, j])
            for d in range(outer):
                total = keep[d, :, where]
                for e in range(1, inner):
                    total = total + yr[e - 1, d, :, where].astype(F32)
                if d:
                    zs[d - 1, :, where] = total.astype(BF16)
                else:
                    own[:, where] = total
            loop(1, outer, lambda d: z_send(j, d).start())

        def line_done(j):
            where = cols(j, cw)
            drain(zr.at[:, :, where], s3_recv.at[ph, j])
            total = own[:, where]
            for d in range(1, outer):
                total = total + zr[d - 1, :, where].astype(F32)
            out[:, where] = tokens[:, where].astype(F32) + total

        def down(low, high):
            hid = (hid_b, hid_a)[ph]
            loop(low, high, lambda j: dn_copy(ph, j).wait())

            def one(j):
                value = jnp.dot(hid[...], dn_slot(ph, j)[...], preferred_element_type=F32)
                if ph == 0:
                    value = value * scale
                count = mine.shape[0]
                first, second = value[:count], value[count:]
                at = cols(j, cb)
                mine[:, at] = jnp.where(core == 0, first, second)
                s1[:, at] = jnp.where(core == 0, second, first).astype(BF16)

            if n > 32:
                loop(low, high, one)
            else:
                for j in range(low, high):
                    one(j)
            loop(low * cb // cw, high * cb // cw, lambda j: pair_copy(j).start())

        return down, pair_done, cross_done, line_done

    far = FAR if chips <= 8 else 0
    near_chunks = chunks - far

    def far_copy(j, s):
        row = lax.rem(p + s // inner, outer)
        place = row * inner + lax.rem(q + s % inner, inner)
        return remote(
            far_out.at[j - near_chunks, s - 1], far_in.at[j - near_chunks, s - 1],
            far_send, far_recv.at[j - near_chunks],
            {"exp": place * 2 + core},
        )

    def far_start(j):
        mine, s1, r1 = back_a[:3]
        where = cols(j, cw)
        remote(
            s1.at[:, where], r1.at[:, where], s1_send.at[1], s1_recv.at[1, j], sibling
        ).wait_recv()
        both = mine[:, where] + r1[:, where].astype(F32)
        for s in range(1, chips):
            far_out[j - near_chunks, s - 1] = both[s * rows_a : (s + 1) * rows_a].astype(BF16)
        back_a[6][:, where] = both[:rows_a]
        loop(1, chips, lambda s: far_copy(j, s).start())

    def far_done(j):
        where = cols(j, cw)
        drain(far_in.at[j - near_chunks], far_recv.at[j - near_chunks])
        total = back_a[6][:, where]
        for s in range(1, chips):
            total = total + far_in[j - near_chunks, s - 1].astype(F32)
        a_out[:, where] = a_in[:, where].astype(F32) + total

    down_b, pair_done_b, cross_done_b, line_done_b = tools(0)
    down_a, pair_done_a, cross_done_a, line_done_a = tools(1)
    mid = chunks // 2

    start_line(0)
    start_own(0)
    for copy in inputs[4:]:
        copy.wait()
    gat_a[0, core] = normed(a_in[...].astype(F32), ag_in[...]).astype(BF16)
    forward_line(0, 1, 2)

    @pl.when(core == 0)
    def _():
        start_line(1)

    forward_line(0, 2, outer)

    @pl.when(core == 1)
    def _():
        start_line(1)

    start_own(1)
    start_line(2)
    forward_cross(0)
    forward_line(1)
    gathered(0)

    def after_b(i):
        start_gu(1, 2 * i)
        start_gu(1, 2 * i + 1)

        @pl.when(i == 0)
        def _():
            forward_cross(1)
            start_own(2)
            forward_line(2)
            gathered(1)

        @pl.when(i == 1)
        def _():
            forward_cross(2)

    hid_b[...] = hidden(0, after_b)
    tables = rows_of(0, pl.ds(width, LANES)) + rows_of(0, pl.ds(width + LANES, LANES))
    chosen = lax.broadcasted_iota(jnp.int32, tables.shape, 1) == expert
    scale = jnp.sum(jnp.where(chosen, tables, 0.0), axis=1, keepdims=True)
    down_b(0, slots // 2)
    loop(slots // 2, slots, lambda j: dn_copy(1, j).start())
    gathered(2)

    def after_a(i):
        @pl.when(i == 0)
        def _():
            loop(mid, chunks, pair_done_b)

        @pl.when(i == steps - 2)
        def _():
            loop(0, mid, cross_done_b)

    down_b(slots // 2, slots)
    loop(0, mid, pair_done_b)
    hid_a[...] = hidden(1, after_a)
    loop(mid, chunks - 1, cross_done_b)
    def pair_sum_a(j):
        (pair_done_a if j < near_chunks else far_start)(j)

    for j in range(chunks):
        down_a(j, j + 1)
        if j == 0:
            loop(chunks - 1, chunks, cross_done_b)
        else:
            pair_sum_a(j - 1)
    loop(0, mid, line_done_b)
    pair_sum_a(chunks - 1)
    loop(mid, chunks, line_done_b)
    loop(0, near_chunks, cross_done_a)
    loop(0, near_chunks, line_done_a)
    loop(near_chunks, chunks, far_done)

    for t in range(3):
        def sent(count):
            if t < 2:
                return gat_b.at[pl.ds(0, count), 0, :, spans[t]]
            return gat_a.at[pl.ds(0, count), 0]

        drain(sent(outer - 1), gz_send.at[t])
        drain(sent(outer * (inner - 1)), gy_send.at[t])
        drain(sent(chips), gc_send.at[t])
    for ph in range(2):
        s1, ys, zs = (back_b, back_a)[ph][1], (back_b, back_a)[ph][4], (back_b, back_a)[ph][7]
        drain(s1, s1_send.at[ph])
        near = pl.ds(0, (chunks, near_chunks)[ph] * cw)
        if (chunks, near_chunks)[ph]:
            drain(ys.at[:, :, :, near], s2_send.at[ph])
            drain(zs.at[:, :, near], s3_send.at[ph])
    if far:
        drain(far_out, far_send)


def finish(sum_a, sum_b, a_out, b_out):
    a_out[...] = sum_a[...].astype(BF16)
    b_out[...] = sum_b[...].astype(BF16)


def shards(
    a_tokens, a_gain, dense_gate, dense_up, dense_down, b_tokens, b_gain, expert_ids,
    route_weights, expert_gate, expert_up, expert_down,
):
    n = lax.axis_size("exp")
    chips = n // 2
    outer, inner = factor(chips)
    ra, width = a_tokens.shape
    rb = b_tokens.shape[0]
    fd = dense_gate.shape[1]
    es = expert_gate.shape[2]
    kq = width // 4
    kc = pick(kq, (256, 128))
    cb = cw = width // 4
    steps, slots = width // kq, width // cb
    extra_width = width + 2 * LANES
    most = n * max(ra, rb)

    def back(rows, span):
        return [
            pltpu.VMEM((chips * rows, span), F32),
            pltpu.VMEM((chips * rows, span), BF16),
            pltpu.VMEM((chips * rows, span), BF16),
            pltpu.VMEM((outer, rows, span), F32),
            pltpu.VMEM((inner - 1, outer, rows, span), BF16),
            pltpu.VMEM((inner - 1, outer, rows, span), BF16),
            pltpu.VMEM((rows, span), F32),
            pltpu.VMEM((outer - 1, rows, span), BF16),
            pltpu.VMEM((outer - 1, rows, span), BF16),
        ]

    vmem = pl.BlockSpec(memory_space=pltpu.VMEM)
    hbm = pl.BlockSpec(memory_space=pl.ANY)
    dma = pltpu.SemaphoreType.DMA
    weights = 3 * width * (fd + es)
    gains = (a_gain.reshape(1, width), b_gain.reshape(1, width))
    sums = pl.pallas_call(
        functools.partial(kernel, n, kq, kc, cb, cw),
        out_shape=(
            pltpu.VMEM(a_tokens.shape, F32),
            pltpu.VMEM(b_tokens.shape, F32),
        ),
        in_specs=[hbm] * 12,
        out_specs=(vmem, vmem),
        scratch_shapes=[
            pltpu.VMEM(a_tokens.shape, BF16),
            pltpu.VMEM((1, width), F32),
            pltpu.VMEM(b_tokens.shape, BF16),
            pltpu.VMEM((1, width), F32),
            pltpu.VMEM(expert_ids.shape, jnp.int32),
            pltpu.VMEM(route_weights.shape, F32),
            pltpu.VMEM((2, steps, kq, max(fd, es)), BF16),
            pltpu.VMEM((slots + slots // 2, max(fd, es), cb), BF16),
            pltpu.VMEM((chips, 2, rb, extra_width), BF16),
            pltpu.VMEM((chips, 2, ra, width), BF16),
            pltpu.VMEM((most, max(fd, es)), F32),
            pltpu.VMEM((most, max(fd, es)), F32),
            pltpu.VMEM((n * rb, es), BF16),
            pltpu.VMEM((n * ra, fd), BF16),
            back(rb, width),
            back(ra, width),
            pltpu.VMEM((FAR, chips - 1 if chips <= 8 else 1, ra, cw), BF16),
            pltpu.VMEM((FAR, chips - 1 if chips <= 8 else 1, ra, cw), BF16),
            dma((6,)),
            dma((2, steps)),
            dma((slots + slots // 2,)),
            dma((3,)),
            dma((3, outer)),
            dma((3,)),
            dma((3, chips)),
            dma((3,)),
            dma((3,)),
            dma((2,)),
            dma((2, width // cw)),
            dma((2,)),
            dma((2, width // cw)),
            dma((2,)),
            dma((2, width // cw)),
            dma,
            dma((FAR,)),
        ],
        compiler_params=pltpu.CompilerParams(
            collective_id=0, has_side_effects=True, vmem_limit_bytes=66400000
        ),
        cost_estimate=pl.CostEstimate(
            flops=2 * n * max(ra, rb) * weights, bytes_accessed=2 * weights, transcendentals=0
        ),
    )(
        a_tokens, gains[0], b_tokens, gains[1], expert_ids, route_weights,
        dense_gate, dense_up, dense_down, expert_gate, expert_up, expert_down,
    )
    return pl.pallas_call(
        finish,
        out_shape=(
            jax.ShapeDtypeStruct(a_tokens.shape, BF16),
            jax.ShapeDtypeStruct(b_tokens.shape, BF16),
        ),
        in_specs=[vmem] * 2,
        out_specs=(vmem, vmem),
    )(*[pltpu.with_memory_space_constraint(x, pltpu.VMEM) for x in sums])


def solution(mesh):
    return jax.shard_map(
        shards,
        mesh=mesh,
        in_specs=(
            P(("rep", "exp"), None),
            P(),
            P(None, "exp"),
            P(None, "exp"),
            P("exp", None),
            P(("rep", "exp"), None),
            P(),
            P(("rep", "exp"), None),
            P(("rep", "exp"), None),
            P("exp", None, None),
            P("exp", None, None),
            P("exp", None, None),
        ),
        out_specs=(P(("rep", "exp"), None), P(("rep", "exp"), None)),
        check_vma=False,
    )
```
